32 devices in a mesh: slab: 16 (over z, y, x), blk: 2 (over core).
Axes of the slice: x: 2, y: 2, z: 4, core: 2. Of those that a mesh axis runs over, the one named last changes fastest.
Arguments:
- slip_rate: float32 [32768], P('slab'), may hold values from 0.1 to 3
- log_state: float32 [32768], P('slab'), may hold values from -1 to 1
- friction_a: float32 [32768], P('slab'), may hold values from 0.2 to 1
- friction_b: float32 [32768], P('slab'), may hold values from 0.2 to 1
- normal_stress: float32 [32768], P('slab'), may hold values from 2 to 4
- leak_rate: float32 [32768], P('slab'), may hold values from 0.5 to 2
- corner: int32 [3, 32768], P(None, 'slab'), may hold values from 0 to 1022, as said below
- fraction: float32 [3, 32768], P(None, 'slab'), may hold values from 0 to 1
- near_blocks: bfloat16 [64, 3, 512, 512], P(('slab', 'blk')), may hold values from -0.15625 to 0.15625
- row_basis: bfloat16 [24, 32768], P(None, 'slab'), may hold values from -1.25 to 1.25
- col_basis: bfloat16 [24, 32768], P(None, 'slab'), may hold values from -0.25 to 0.25
- far_row: int32 [32768], P(('slab', 'blk')), may hold values from 0 to 3
- far_col: int32 [32768], P(('slab', 'blk')), may hold values from 0 to 63, as said below
- far_rank: int32 [32768], P(('slab', 'blk')), may hold values from 0 to 24, as said below
- far_coupling: bfloat16 [24, 24, 32768], P(None, None, ('slab', 'blk')), may hold values from -0.078125 to 0.078125
- pressure: float32 [32, 512, 1024], P('slab', 'blk'), may hold values from -1 to 1
- region: int32 [32, 512, 1024], P('slab', 'blk'), may hold values from 0 to 15
- perm_table: float32 [16], replicated, may hold values from 0.05 to 1
Outputs:
- slip_accel: float32 [32768], P('slab')
- state_rate: float32 [32768], P('slab')
- pressure_rate: float32 [32, 512, 1024], P('slab', 'blk')
The draws below stay inside these ranges and needn't reach their ends.
Inputs may be any that keep to these rules, and one draw needn't show every extreme that they name: corner[0, f] equals 2 * (f // 2048), the first plane of the slab that holds cell f; corner[1, f] is at most 510 and corner[2, f] at most 1022. far_col[s] differs by 2 or more (cyclically over 64 clusters) from the slot's row cluster 4 * (s // 2048) + far_row[s]. `far_rank`: slots with rank 0 are empty; the live slots of a device come first, and some device has all 1024 slots live.
All inputs are finite; a program needn't handle non-finite values.
Results may differ from the reference program's by a relative error of at most 0.0022.
Values may be sent and summed in bfloat16 or wider, within the bound.
No kernel may reach another device: no remote copies, remote signals or barrier semaphores. Data moves between devices by JAX's collectives and lax.ppermute only.
A program may use at most 64 MiB of HBM per device.

```python
import math
import jax
import jax.numpy as jnp
from jax import lax

CS = 512
RANK = 24
REGIONS = 16
CL = 4
FB = 1024
CX = 2
CY = 256
CZ = 1024
C = 64
FAULT = 32768
SLOTS = 32768
NX = 32
NY = 512
NZ = 1024
N_SLAB = 16
N_BLK = 2


def far_slots(key):
    total = N_SLAB * N_BLK * FB
    clusters = CL * N_SLAB
    slot = jnp.arange(total, dtype=jnp.int32)
    owner = slot // FB
    rows = jax.random.randint(jax.random.fold_in(key, 11), (total,), 0, CL)
    global_row = owner // N_BLK * CL + rows
    offset = jax.random.randint(jax.random.fold_in(key, 12), (total,), 0, clusters - 3)
    cols = (global_row + 2 + offset) % clusters
    return (rows.astype(jnp.int32), cols.astype(jnp.int32))


def draw_far_row(key, part):
    return far_slots(key)[0]


def draw_far_col(key, part):
    return far_slots(key)[1]


def draw_far_rank(key, part):
    devices = N_SLAB * N_BLK
    total = devices * FB
    slot = jnp.arange(total, dtype=jnp.int32)
    live = jax.random.randint(jax.random.fold_in(key, 13), (devices,), FB // 8, FB + 1)
    chosen = jax.random.randint(jax.random.fold_in(key, 15), (), 0, devices)
    live = jnp.where(jnp.arange(devices, dtype=jnp.int32) == chosen, FB, live)
    ranks = jax.random.randint(jax.random.fold_in(key, 14), (total,), 1, RANK + 1)
    return jnp.where(slot % FB < live[slot // FB], ranks, 0).astype(jnp.int32)


def draw_corner(key, part):
    cells = CL * N_SLAB * CS
    position = jnp.arange(cells, dtype=jnp.int32)
    slab_group = position // (CL * CS)
    first = slab_group * CX + jax.random.randint(jax.random.fold_in(key, 21), (cells,), 0, CX - 1)
    second = jax.random.randint(jax.random.fold_in(key, 22), (cells,), 0, CY * N_BLK - 1)
    third = jax.random.randint(jax.random.fold_in(key, 23), (cells,), 0, CZ - 1)
    return jnp.stack([first, second, third]).astype(jnp.int32)


def set_ends(result, key, low, top_value):
    longest = result.shape.index(max(result.shape))
    spots = []
    for shift in (0, 1):
        where = [jax.random.randint(jax.random.fold_in(key, axis), (), 0, length) for axis, length in enumerate(result.shape)]
        where[longest] = (where[longest] + shift) % result.shape[longest]
        spots.append(tuple(where))
    return result.at[spots[0]].set(low).at[spots[1]].set(top_value)


def shard_levels(stream_key, shape, shards, smallest, top_value):
    factor_of, own = 1.0, jax.random.fold_in(stream_key, 6)
    for axis_at, shards_of in shards:
        heights = jnp.exp(jax.random.uniform(jax.random.fold_in(own, axis_at), (shards_of,), jnp.float32, smallest / len(shards), top_value / len(shards)))
        factor_of = factor_of * jnp.repeat(heights, shape[axis_at] // shards_of).reshape([-1 if axis == axis_at else 1 for axis in range(len(shape))])
    return factor_of


def gaussian(key, dims, scale, reach, cuts=(), kind=jnp.bfloat16):
    entries = scale * jax.random.normal(key, dims, jnp.float32)
    if cuts:
        entries = entries * shard_levels(key, dims, cuts, -0.22, 0.18)
    return jnp.clip(entries, -reach, reach).astype(kind)


def setup_inputs(seed: int = 0) -> dict:
    keys = jax.random.split(jax.random.key(seed), 19)
    return {
        "slip_rate": jnp.clip(jnp.exp(math.log(3.0) - 3.4011974 * jax.random.uniform(keys[0], (FAULT,), jnp.float32) ** shard_levels(keys[0], (FAULT,), ((0, 16),), -0.2, 0.2)), 0.1, 3.0),
        "log_state": jnp.clip(jax.random.uniform(keys[1], (FAULT,), jnp.float32, -1.0, 1.0) * shard_levels(keys[1], (FAULT,), ((0, 16),), -0.4, 0.0), -1.0, 1.0),
        "friction_a": jnp.clip(jnp.exp(math.log(1.0) - 1.609438 * jax.random.uniform(keys[2], (FAULT,), jnp.float32) ** shard_levels(keys[2], (FAULT,), ((0, 16),), -0.2, 0.2)), 0.2, 1.0),
        "friction_b": jnp.clip(jnp.exp(math.log(1.0) - 1.609438 * jax.random.uniform(keys[3], (FAULT,), jnp.float32) ** shard_levels(keys[3], (FAULT,), ((0, 16),), -0.2, 0.2)), 0.2, 1.0),
        "normal_stress": jnp.clip(2.0 + 2.0 * jax.random.uniform(keys[4], (FAULT,), jnp.float32) ** shard_levels(keys[4], (FAULT,), ((0, 16),), -0.2, 0.2), 2.0, 4.0),
        "leak_rate": jnp.clip(jnp.exp(math.log(2.0) - 1.3862944 * jax.random.uniform(keys[5], (FAULT,), jnp.float32) ** shard_levels(keys[5], (FAULT,), ((0, 16),), -0.2, 0.2)), 0.5, 2.0),
        "corner": draw_corner(jax.random.fold_in(keys[18], 71), 0),
        "fraction": jnp.clip(1.0 * jax.random.uniform(keys[7], (3, FAULT), jnp.float32) ** shard_levels(keys[7], (3, FAULT), ((1, 16),), -0.2, 0.2), 0.0, 1.0),
        "near_blocks": gaussian(keys[8], (C, 3, CS, CS), (3 * CS) ** -0.5, 0.15625, ((0, 32),)),
        "row_basis": gaussian(keys[9], (RANK, FAULT), RANK ** -0.5, 1.25, ((1, 16),)),
        "col_basis": gaussian(keys[10], (RANK, FAULT), CS ** -0.5, 0.25, ((1, 16),)),
        "far_row": draw_far_row(jax.random.fold_in(keys[18], 71), 0),
        "far_col": draw_far_col(jax.random.fold_in(keys[18], 71), 0),
        "far_rank": draw_far_rank(jax.random.fold_in(keys[18], 71), 0),
        "far_coupling": gaussian(keys[14], (RANK, RANK, SLOTS), (RANK * FB * N_BLK // (2 * CL)) ** -0.5, 0.078125, ((2, 32),)),
        "pressure": gaussian(keys[15], (NX, NY, NZ), 0.25, 1.0, ((0, 16), (1, 2)), jnp.float32),
        "region": set_ends(jax.random.randint(keys[16], (NX, NY, NZ), 0, REGIONS), jax.random.fold_in(keys[16], 1), 0, REGIONS - 1).astype(jnp.int32),
        "perm_table": jnp.clip(jnp.exp(jax.random.uniform(keys[17], (REGIONS,), jnp.float32, math.log(0.05), math.log(1.0))), 0.05, 1.0),
    }


def corner_list(corner, fraction):
    listed = []
    for shift_x in (0, 1):
        for shift_y in (0, 1):
            for shift_z in (0, 1):
                factor_x = fraction[0] if shift_x else 1.0 - fraction[0]
                factor_y = fraction[1] if shift_y else 1.0 - fraction[1]
                factor_z = fraction[2] if shift_z else 1.0 - fraction[2]
                weight = factor_x * factor_y * factor_z
                listed.append((corner[0] + shift_x, corner[1] + shift_y, corner[2] + shift_z, weight))
    return listed


def stencil(padded_p, padded_k):
    centre_p = padded_p[1:-1, 1:-1, 1:-1]
    centre_k = padded_k[1:-1, 1:-1, 1:-1]
    summed = jnp.zeros_like(centre_p)
    for slices in ((slice(2, None), slice(1, -1), slice(1, -1)), (slice(0, -2), slice(1, -1), slice(1, -1)),
                   (slice(1, -1), slice(2, None), slice(1, -1)), (slice(1, -1), slice(0, -2), slice(1, -1)),
                   (slice(1, -1), slice(1, -1), slice(2, None)), (slice(1, -1), slice(1, -1), slice(0, -2))):
        other_k = padded_k[slices]
        other_p = padded_p[slices]
        summed = summed + 2.0 * centre_k * other_k / (centre_k + other_k) * (other_p - centre_p)
    return summed


def reference(slip_rate, log_state, friction_a, friction_b, normal_stress, leak_rate, corner, fraction,
              near_blocks, row_basis, col_basis, far_row, far_col, far_rank, far_coupling, pressure, region,
              perm_table):
    slip_low = slip_rate.astype(jnp.bfloat16)
    by_cluster = jnp.pad(slip_low.reshape(C, CS), ((1, 1), (0, 0)))

    def near_row(which):
        window = lax.dynamic_slice_in_dim(by_cluster, which, 3, 0).astype(jnp.float32)
        blocks = near_blocks[which].astype(jnp.float32)
        return jnp.einsum('jxy,jy->x', blocks, window)

    near_traction = lax.map(near_row, jnp.arange(C, dtype=jnp.int32))
    moments = jnp.einsum('acx,cx->ac', col_basis.reshape(RANK, C, CS).astype(jnp.float32),
                         slip_low.reshape(C, CS).astype(jnp.float32),
                         precision=lax.Precision.HIGHEST).astype(jnp.bfloat16)
    ranks_iota = lax.broadcasted_iota(jnp.int32, (RANK, FB), 0)
    cluster_iota = lax.broadcasted_iota(jnp.int32, (C, FB), 0)

    def add_device(totals, device):
        start = (device * FB).astype(jnp.int32)
        coupling = lax.dynamic_slice_in_dim(far_coupling, start, FB, 2).astype(jnp.float32)
        cols = lax.dynamic_slice_in_dim(far_col, start, FB, 0)
        rows = lax.dynamic_slice_in_dim(far_row, start, FB, 0)
        ranks = lax.dynamic_slice_in_dim(far_rank, start, FB, 0)
        picked = jnp.take(moments, cols, axis=1).astype(jnp.float32)
        masked = jnp.where(ranks_iota < ranks[None, :], picked, jnp.float32(0.0))
        block = jnp.einsum('akf,kf->af', coupling, masked)
        global_row = (device // N_BLK).astype(jnp.int32) * CL + rows
        one_hot = (global_row[None, :] == cluster_iota).astype(jnp.float32)
        return totals + jnp.dot(block, one_hot.T, precision=lax.Precision.HIGHEST), None

    totals, _ = lax.scan(add_device, jnp.zeros((RANK, C), jnp.float32),
                         jnp.arange(N_SLAB * N_BLK, dtype=jnp.int32))
    far_traction = jnp.einsum('acx,ac->cx', row_basis.reshape(RANK, C, CS).astype(jnp.float32), totals,
                              precision=lax.Precision.HIGHEST)
    traction = (near_traction + far_traction).reshape(FAULT)

    listed = corner_list(corner, fraction)
    fault_pressure = jnp.zeros((FAULT,), jnp.float32)
    source = jnp.zeros((NX, NY, NZ), jnp.float32)
    flow = leak_rate * slip_rate
    for place_x, place_y, place_z, weight in listed:
        fault_pressure = fault_pressure + weight * pressure[place_x, place_y, place_z]
        source = source.at[place_x, place_y, place_z].add(weight * flow)
    effective = normal_stress - fault_pressure
    state_rate = jnp.exp(-log_state) - slip_rate
    slip_accel = (traction - effective * friction_b * state_rate) / (effective * friction_a / slip_rate + 0.5)

    permeability = jnp.zeros((NX, NY, NZ), jnp.float32)
    for which in range(REGIONS):
        permeability = jnp.where(region == which, perm_table[which], permeability)
    padded_p = jnp.pad(pressure, 1)
    padded_k = jnp.pad(permeability, 1)
    pressure_rate = source + stencil(padded_p, padded_k)
    return slip_accel, state_rate, pressure_rate
```

```python
import functools

import jax
import jax.numpy as jnp
from jax import lax
from jax.experimental import pallas as pl
from jax.experimental.pallas import tpu as pltpu
from jax.sharding import PartitionSpec as P

VMEM = pltpu.MemorySpace.VMEM
SMEM = pltpu.MemorySpace.SMEM
SPLIT = (8,)


def row_chunks(rows):
    sizes = [rows * part // sum(SPLIT) for part in SPLIT]
    starts = [sum(sizes[:i]) for i in range(len(sizes))]
    return list(zip(starts, sizes))


def lookup(table, index):
    height, width = index.shape
    table = jnp.concatenate([table] * (height // 8), axis=0)
    parts = [
        jnp.take_along_axis(table, index[:, at : at + 128], axis=1) for at in range(0, width, 128)
    ]
    return jnp.concatenate(parts, axis=1)


def prepare_kernel(
    chunks, clusters, core_ref, p_ref, region_ref, p_edge_ref, region_edge_ref, slip_ref, basis_ref, *outs
):
    edge_ref, message_ref = outs[-2:]
    f32, bf16 = jnp.float32, jnp.bfloat16
    planes = p_edge_ref.shape[0]
    for (start, size), out in zip(chunks, outs):
        rows = pl.ds(start, size)
        out[0] = p_ref[0, rows, :].astype(bf16)
        out[1] = region_ref[0, rows, :].astype(f32).astype(bf16)
    low = core_ref[0] != 0
    for plane in range(planes):
        block, kind = p_edge_ref[plane], region_edge_ref[plane].astype(f32)
        edge_ref[plane : plane + 1, :] = jnp.where(low, block[0:1, :], block[7:8, :])
        edge_ref[planes + plane : planes + plane + 1, :] = jnp.where(low, kind[0:1, :], kind[7:8, :])
    cells = slip_ref.shape[1]
    size = cells // clusters
    per = size // 128
    slip = slip_ref[...].astype(bf16).astype(f32)
    lines = [slip[:, at : at + 128] for at in range(0, size, 128)]
    lines += [slip[:, at : at + 128] for at in range(cells - size, cells, 128)]
    rank = basis_ref.shape[0]
    for cluster in range(clusters):
        part = slip[:, cluster * size : (cluster + 1) * size].astype(bf16)
        moment = lax.dot_general(
            jnp.broadcast_to(part, (16, size)),
            basis_ref[:, cluster * size : (cluster + 1) * size],
            (((1,), (1,)), ((), ())),
            preferred_element_type=f32,
        )[0:1, :]
        lines.append(jnp.concatenate([moment, jnp.zeros((1, 128 - rank), f32)], axis=1))
    height = message_ref.shape[1]
    lines.append(jnp.zeros((height - len(lines), 128), f32))
    message = jnp.concatenate(lines, axis=0).astype(bf16)
    for slab in range(message_ref.shape[0]):
        message_ref[slab] = message


def prepare(pressure, region, slip, basis, core, chunks, clusters, slabs):
    planes, rows, width = pressure.shape
    cells = slip.shape[1]
    lines = 2 * (cells // clusters // 128) + clusters
    height = -(-lines // 16) * 16
    plane = pl.BlockSpec((1, rows, width), lambda i, core: (planes - 1, 0, 0))
    edge = pl.BlockSpec((planes, 8, width), lambda i, core: (0, (1 - core[0]) * (rows // 8 - 1), 0))
    full = lambda shape: pl.BlockSpec(shape, lambda i, core: (0,) * len(shape))
    shapes = [((2, size, width), jnp.bfloat16) for _, size in chunks]
    shapes += [((2 * planes, width), jnp.float32), ((slabs, height, 128), jnp.bfloat16)]
    return pl.pallas_call(
        functools.partial(prepare_kernel, chunks, clusters),
        grid_spec=pltpu.PrefetchScalarGridSpec(
            num_scalar_prefetch=1,
            grid=(1,),
            in_specs=[plane, plane, edge, edge, full(slip.shape), full(basis.shape)],
            out_specs=[full(shape) for shape, _ in shapes],
        ),
        out_shape=[jax.ShapeDtypeStruct(*shape) for shape in shapes],
        name="prepare",
    )(core, pressure, region, pressure, region, slip, basis)


def cells_kernel(start_ref, p_ref, corner_ref, fraction_ref, slip_ref, leak_ref, sampled_ref, source_ref, field):
    planes, rows, width = p_ref.shape
    cells = corner_ref.shape[1]
    step = pl.program_id(0)
    f32, bf16 = jnp.float32, jnp.bfloat16

    @pl.when(step == 0)
    def _():
        field[...] = p_ref[...].astype(bf16)

    frac = fraction_ref[...]
    at_y = corner_ref[1:2, :] - start_ref[0]
    at_z = corner_ref[2:3, :]
    high_z = frac[2:3, :]
    low_z = 1.0 - high_z
    low_hi, high_hi = low_z.astype(bf16).astype(f32), high_z.astype(bf16).astype(f32)
    iota = lax.broadcasted_iota(jnp.int32, (width, cells), 0)
    here, above = iota == at_z, iota == at_z + 1
    zero = jnp.float32(0.0)
    z_hi = jnp.where(here, low_hi, jnp.where(above, high_hi, zero)).astype(bf16)
    z_lo = jnp.where(here, low_z - low_hi, jnp.where(above, high_z - high_hi, zero)).astype(bf16)
    iota_y = lax.broadcasted_iota(jnp.int32, (rows, cells), 0)
    weight_y = jnp.where(
        iota_y == at_y, 1.0 - frac[1:2, :], jnp.where(iota_y == at_y + 1, frac[1:2, :], zero)
    )
    flow = slip_ref[...] * leak_ref[...]
    total = jnp.zeros((1, cells), f32)
    for plane in range(2):
        weight_x = frac[0:1, :] if plane else 1.0 - frac[0:1, :]
        along = jnp.dot(field[plane], z_hi, preferred_element_type=f32)
        total = total + weight_x * jnp.sum(weight_y * along, axis=0, keepdims=True)
        scaled = (weight_y * (weight_x * flow)).astype(bf16)
        dims = (((1,), (1,)), ((), ()))
        spread = lax.dot_general(scaled, z_hi, dims, preferred_element_type=f32)
        spread = spread + lax.dot_general(scaled, z_lo, dims, preferred_element_type=f32)

        @pl.when(step == 0)
        def _():
            source_ref[plane] = spread

        @pl.when(step != 0)
        def _():
            source_ref[plane] = source_ref[plane] + spread

    sampled_ref[...] = total


def cells(pressure, corner, fraction, slip, leak, y_start, block):
    planes, rows, width = pressure.shape
    count = corner.shape[1]
    vec = lambda n: pl.BlockSpec((n, block), lambda i: (0, i))
    whole = pl.BlockSpec((planes, rows, width), lambda i: (0, 0, 0))
    return pl.pallas_call(
        cells_kernel,
        grid=(count // block,),
        in_specs=[pl.BlockSpec(memory_space=SMEM), whole, vec(3), vec(3), vec(1), vec(1)],
        out_specs=[vec(1), whole],
        out_shape=[
            jax.ShapeDtypeStruct((1, count), jnp.float32),
            jax.ShapeDtypeStruct(pressure.shape, jnp.float32),
        ],
        scratch_shapes=[pltpu.VMEM(pressure.shape, jnp.bfloat16)],
        cost_estimate=pl.CostEstimate(
            flops=6 * planes * rows * width * count, bytes_accessed=4 * pressure.size * 2, transcendentals=0
        ),
        name="cells",
    )(y_start, pressure, corner, fraction, slip, leak)


def stencil_kernel(
    core_ref, table_ref, p_ref, p_before, p_after, k_ref, k_before, k_after, edge_ref, source_ref, low_ref,
    out_ref, pad_p, pad_r,
):
    planes, rows, width = p_ref.shape
    f32 = jnp.float32
    far = jnp.float32(jnp.inf)
    strips = rows // 16
    core = core_ref[0]
    step, last = pl.program_id(0), pl.num_programs(0) - 1
    table = table_ref[...]
    outside = jnp.full((8, width), far, f32)
    for plane in range(planes):
        pad_p[plane, 0:8, :] = p_before[plane]
        pad_r[plane, 0:8, :] = lookup(table, k_before[plane])
        pad_p[plane, rows + 8 : rows + 16, :] = p_after[plane]
        pad_r[plane, rows + 8 : rows + 16, :] = lookup(table, k_after[plane])

    for at_step, at, mine in ((0, 0, core != 0), (last, rows + 8, core == 0)):

        @pl.when(step == at_step)
        def _():
            for plane in range(planes):
                edge_p = jnp.broadcast_to(edge_ref[plane : plane + 1, :], (8, width))
                edge_k = edge_ref[planes + plane : planes + plane + 1, :].astype(jnp.int32)
                edge_r = lookup(table, jnp.broadcast_to(edge_k, (8, width)))
                pad_p[plane, at : at + 8, :] = edge_p
                pad_r[plane, at : at + 8, :] = jnp.where(mine, edge_r, outside)

    def fill(s, carry):
        at = pl.multiple_of(s * 8, 8)
        to = pl.multiple_of(s * 8 + 8, 8)
        for plane in range(planes):
            pad_p[plane, pl.ds(to, 8), :] = p_ref[plane, pl.ds(at, 8), :]
            pad_r[plane, pl.ds(to, 8), :] = lookup(table, k_ref[plane, pl.ds(at, 8), :])
        return carry

    lax.fori_loop(0, rows // 8, fill, 0)
    lane = lax.broadcasted_iota(jnp.int32, (8, width), 1)
    sub = lax.broadcasted_iota(jnp.int32, (8, width), 0)

    def face(p, r, p_next, r_next):
        return 2.0 / (r + r_next) * (p_next - p)

    def y_face(plane, at):
        p, r = pad_p[plane, pl.ds(at, 8), :], pad_r[plane, pl.ds(at, 8), :]
        after = pl.multiple_of(at + 8, 8)
        pn, rn = pad_p[plane, pl.ds(after, 8), :], pad_r[plane, pl.ds(after, 8), :]
        pn = pltpu.roll(jnp.where(sub == 0, pn, p), 7, 0)
        rn = pltpu.roll(jnp.where(sub == 0, rn, r), 7, 0)
        return p, r, face(p, r, pn, rn)

    def strip(to, low, carry):
        at = pl.multiple_of(to + 8, 8)
        after = []
        sums, ps, rs = [], [], []
        for plane in range(planes):
            p, r, fy = y_face(plane, at)
            below = pltpu.roll(jnp.where(sub == 7, carry[plane], fy), 1, 0)
            after.append(fy)
            pz = pltpu.roll(p, width - 1, 1)
            rz = jnp.where(lane == width - 1, far, pltpu.roll(r, width - 1, 1))
            fz = face(p, r, pz, rz)
            sums.append(fy - below + (fz - pltpu.roll(fz, 1, 1)))
            ps.append(p)
            rs.append(r)
        for plane in range(planes - 1):
            fx = face(ps[plane], rs[plane], ps[plane + 1], rs[plane + 1])
            sums[plane] = sums[plane] + fx
            sums[plane + 1] = sums[plane + 1] - fx
        sums[0] = sums[0] + low
        for plane in range(planes):
            out_ref[plane, pl.ds(to, 8), :] = source_ref[plane, pl.ds(to, 8), :] + sums[plane]
        return tuple(after)

    def body(s, carry):
        to = pl.multiple_of(s * 16, 16)
        low = low_ref[pl.ds(to, 16), :].astype(f32)
        carry = strip(to, low[:8], carry)
        return strip(pl.multiple_of(to + 8, 8), low[8:], carry)

    first = tuple(y_face(plane, 0)[2] for plane in range(planes))
    lax.fori_loop(0, strips, body, first)


def local_stencil(pressure, region, edge, source, low, table, core, block):
    planes, rows, width = pressure.shape
    smem = pl.BlockSpec(memory_space=SMEM)
    part = pl.BlockSpec((planes, block, width), lambda i: (0, i, 0))
    eighth = block // 8
    before = pl.BlockSpec((planes, 8, width), lambda i: (0, jnp.maximum(i * eighth - 1, 0), 0))
    after = pl.BlockSpec(
        (planes, 8, width), lambda i: (0, jnp.minimum((i + 1) * eighth, rows // 8 - 1), 0)
    )
    full = lambda shape: pl.BlockSpec(shape, lambda i: (0,) * len(shape))
    return pl.pallas_call(
        stencil_kernel,
        grid=(rows // block,),
        in_specs=[
            smem, full(table.shape), part, before, after, part, before, after, full(edge.shape), part,
            pl.BlockSpec((block, width), lambda i: (i, 0)),
        ],
        out_specs=part,
        out_shape=jax.ShapeDtypeStruct(pressure.shape, jnp.float32),
        scratch_shapes=[pltpu.VMEM((planes, block + 16, width), jnp.float32)] * 2,
        input_output_aliases={9: 0},
        cost_estimate=pl.CostEstimate(
            flops=200 * pressure.size, bytes_accessed=16 * pressure.size, transcendentals=0
        ),
        name="stencil",
    )(core, table, pressure, pressure, pressure, region, region, region, edge, source, low)


def face_kernel(valid_ref, table_ref, halo_ref, p_ref, region_ref, out_ref):
    valid = valid_ref[0] != 0
    far = jnp.float32(jnp.inf)
    table = table_ref[...]

    def body(s, carry):
        at = pl.multiple_of(s * 16, 16)
        rows = pl.ds(at, 16)
        other_p = halo_ref[0, rows, :].astype(jnp.float32)
        other_r = lookup(table, halo_ref[1, rows, :].astype(jnp.float32).astype(jnp.int32))
        other_r = jnp.where(valid, other_r, far)
        r = lookup(table, region_ref[0, rows, :])
        flux = 2.0 / (r + other_r) * (other_p - p_ref[0, rows, :])
        out_ref[rows, :] = flux.astype(jnp.bfloat16)
        return carry

    lax.fori_loop(0, out_ref.shape[0] // 16, body, 0)


def face_flux(halo, pressure, region, table, valid, start, block):
    size, width = halo.shape[1:]
    smem = pl.BlockSpec(memory_space=SMEM)
    rows = pl.BlockSpec((1, block, width), lambda i: (0, start // block + i, 0))
    return pl.pallas_call(
        face_kernel,
        grid=(size // block,),
        in_specs=[
            smem,
            pl.BlockSpec(table.shape, lambda i: (0, 0)),
            pl.BlockSpec((2, block, width), lambda i: (0, i, 0)),
            rows,
            rows,
        ],
        out_specs=pl.BlockSpec((block, width), lambda i: (i, 0)),
        out_shape=jax.ShapeDtypeStruct((size, width), jnp.bfloat16),
        name="face",
    )(valid, table, halo, pressure, region)


def finish_kernel(sign, flux_ref, acc_ref, out_ref):
    out_ref[0] = acc_ref[0] + sign * flux_ref[...].astype(jnp.float32)


def finish(acc, flux, plane, start, sign, block):
    planes, rows, width = acc.shape
    size = flux.shape[0]
    part = pl.BlockSpec((1, block, width), lambda i: (plane, start // block + i, 0))
    return pl.pallas_call(
        functools.partial(finish_kernel, sign),
        grid=(size // block,),
        in_specs=[pl.BlockSpec((block, width), lambda i: (i, 0)), part],
        out_specs=part,
        out_shape=jax.ShapeDtypeStruct(acc.shape, jnp.float32),
        input_output_aliases={1: 0},
        name="finish",
    )(flux, acc)


def traction_kernel(
    place_ref, got_ref, slip_ref, near_ref, coupling_ref, far_ref, basis_ref, out_ref, *, half_rows
):
    f32, bf16 = jnp.float32, jnp.bfloat16
    core, slab = place_ref[0], place_ref[1]
    slabs = got_ref.shape[0]
    rank, cells = basis_ref.shape
    size = near_ref.shape[2]
    clusters = cells // size
    per = size // 128
    slots = far_ref.shape[1]

    cols, rows, ranks = far_ref[0:1, :], far_ref[1:2, :], far_ref[2:3, :]
    owner, member = cols // clusters, cols % clusters
    slab_iota = lax.broadcasted_iota(jnp.int32, (slabs, slots), 0)
    pick = (slab_iota == owner).astype(f32).astype(bf16)
    picked = jnp.zeros((128, slots), f32)
    for cluster in range(clusters):
        sent = got_ref[:, 2 * per + cluster, :]
        chosen = lax.dot_general(sent, pick, (((0,), (0,)), ((), ())), preferred_element_type=f32)
        picked = jnp.where(member == cluster, chosen, picked)
    rank_iota = lax.broadcasted_iota(jnp.int32, (rank, slots), 0)
    masked = jnp.where(rank_iota < ranks, picked[:rank, :], jnp.float32(0.0))
    lines = []
    for a in range(rank):
        lines.append(jnp.sum(coupling_ref[a].astype(f32) * masked, axis=0, keepdims=True))
    block = jnp.concatenate(lines, axis=0)
    far = []
    for cluster in range(clusters):
        total = jnp.sum(jnp.where(rows == cluster, block, jnp.float32(0.0)), axis=1, keepdims=True)
        basis = basis_ref[:, cluster * size : (cluster + 1) * size].astype(f32)
        far.append(jnp.sum(basis * total, axis=0, keepdims=True))

    def line(slab_at, row):
        parts = [got_ref[pl.ds(slab_at, 1), row + i, :].astype(f32) for i in range(per)]
        return jnp.concatenate(parts, axis=1)

    zero = jnp.zeros((1, size), f32)
    before = jnp.where(slab > 0, line(jnp.maximum(slab - 1, 0), per), zero)
    after = jnp.where(slab < slabs - 1, line(jnp.minimum(slab + 1, slabs - 1), 0), zero)
    slip = slip_ref[...].astype(bf16).astype(f32)
    extended = [before] + [slip[:, c * size : (c + 1) * size] for c in range(clusters)] + [after]
    near = []
    for i in range(half_rows):
        total = jnp.zeros((16, size), f32)
        for j in range(3):
            source = jnp.where(core == 0, extended[i + j], extended[half_rows + i + j])
            total = total + lax.dot_general(
                jnp.broadcast_to(source, (16, size)).astype(bf16),
                near_ref[i, j],
                (((1,), (1,)), ((), ())),
                preferred_element_type=f32,
            )
        near.append(total[0:1, :])
    for cluster in range(clusters):
        mine = (cluster // half_rows) == core
        out_ref[:, cluster * size : (cluster + 1) * size] = far[cluster] + jnp.where(
            mine, near[cluster % half_rows], zero
        )


def traction_share(got, slip, near_blocks, far_coupling, far, row_basis, place):
    vmem, smem = pl.BlockSpec(memory_space=VMEM), pl.BlockSpec(memory_space=SMEM)
    return pl.pallas_call(
        functools.partial(traction_kernel, half_rows=near_blocks.shape[0]),
        in_specs=[smem] + [vmem] * 6,
        out_specs=vmem,
        out_shape=jax.ShapeDtypeStruct(slip.shape, jnp.float32),
        name="traction",
    )(place, got, slip, near_blocks, far_coupling, far, row_basis)


def shards(
    slip_rate,
    log_state,
    friction_a,
    friction_b,
    normal_stress,
    leak_rate,
    corner,
    fraction,
    near_blocks,
    row_basis,
    col_basis,
    far_row,
    far_col,
    far_rank,
    far_coupling,
    pressure,
    region,
    perm_table,
):
    slab = lax.axis_index("slab").astype(jnp.int32)
    core = lax.axis_index("blk").astype(jnp.int32)
    slabs = lax.axis_size("slab")
    planes, rows, width = pressure.shape
    cluster_size = near_blocks.shape[2]
    fault_cells = slip_rate.shape[0]
    clusters = fault_cells // cluster_size
    forward = [(i, i + 1) for i in range(slabs - 1)]
    backward = [(target, source) for source, target in forward]
    swap = [(0, 1), (1, 0)]
    chunks = row_chunks(rows)
    kinds = perm_table.shape[0]
    table = jnp.broadcast_to(jnp.pad(1.0 / perm_table, (0, 128 - kinds)), (8, 128))
    core_1 = core.reshape(1)
    valid = (slab > 0).astype(jnp.int32).reshape(1)
    slip = slip_rate.reshape(1, fault_cells)
    leak = leak_rate.reshape(1, fault_cells)

    *packed, edge, message = prepare(
        pressure, region, slip, col_basis, core_1, chunks, clusters, slabs
    )
    halos = [lax.ppermute(part, "slab", forward) for part in packed]
    edge = lax.ppermute(edge, "blk", swap)
    got = lax.all_to_all(message, "slab", 0, 0, tiled=True)

    sampled, source = cells(
        pressure, corner, fraction, slip, leak, (core * rows).reshape(1), 512
    )

    lows = [
        face_flux(halo, pressure, region, table, valid, start, size)
        for halo, (start, size) in zip(halos, chunks)
    ]
    highs = [lax.ppermute(low, "slab", backward) for low in lows]
    low = lows[0] if len(lows) == 1 else jnp.concatenate(lows, 0)
    rate = local_stencil(pressure, region, edge, source, low, table, core_1, 128)

    far = jnp.stack([far_col, far_row, far_rank])
    place = jnp.stack([core, slab])
    share = traction_share(got, slip, near_blocks, far_coupling, far, row_basis, place)
    shares = jnp.concatenate([share, sampled], 0)
    shares = shares + lax.ppermute(shares, "blk", swap)
    traction, fault_pressure = shares[0], shares[1]
    effective = normal_stress - fault_pressure
    state_rate = jnp.exp(-log_state) - slip_rate
    slip_accel = (traction - effective * friction_b * state_rate) / (
        effective * friction_a / slip_rate + 0.5
    )
    for high, (start, size) in zip(highs, chunks):
        rate = finish(rate, high, planes - 1, start, -1.0, size)
    return (slip_accel, state_rate, rate)


def solution(mesh):
    placed = (
        P("slab"),
        P("slab"),
        P("slab"),
        P("slab"),
        P("slab"),
        P("slab"),
        P(None, "slab"),
        P(None, "slab"),
        P(("slab", "blk"), None, None, None),
        P(None, "slab"),
        P(None, "slab"),
        P(("slab", "blk")),
        P(("slab", "blk")),
        P(("slab", "blk")),
        P(None, None, ("slab", "blk")),
        P("slab", "blk", None),
        P("slab", "blk", None),
        P(),
    )
    return jax.shard_map(
        shards,
        mesh=mesh,
        in_specs=placed,
        out_specs=(P("slab"), P("slab"), P("slab", "blk", None)),
        check_vma=False,
    )
```

```python
import functools

import jax
import jax.numpy as jnp
from jax import lax
from jax.experimental import pallas as pl
from jax.experimental.pallas import tpu as pltpu
from jax.sharding import PartitionSpec as P


VMEM = pltpu.MemorySpace.VMEM
SMEM = pltpu.MemorySpace.SMEM
UNROLL = 32
PARTS = (4, 4)
VMEM_OUT = pltpu.VMEM


def row_parts(rows):
    sizes = [rows * part // sum(PARTS) for part in PARTS]
    return [(sum(sizes[:i]), size) for i, size in enumerate(sizes)]


def params(megabytes):
    return pltpu.CompilerParams(vmem_limit_bytes=megabytes << 20)


def in_hbm(x):
    return pltpu.with_memory_space_constraint(x, pltpu.MemorySpace.HBM)


def make_table(values_ref):
    lane = lax.broadcasted_iota(jnp.int32, (8, 128), 1)
    table = jnp.ones((8, 128), jnp.float32)
    for i in range(values_ref.shape[0]):
        table = jnp.where(lane == i, values_ref[i], table)
    return 1.0 / table


def lookup(table, index):
    height, width = index.shape
    table = jnp.concatenate([table] * (height // 8), axis=0)
    parts = [
        jnp.take_along_axis(table, index[:, at : at + 128], axis=1) for at in range(0, width, 128)
    ]
    return jnp.concatenate(parts, axis=1)


def prepare_kernel(
    clusters, core_ref, slab_ref, p_hbm, k_hbm, slip_hbm, basis_hbm, halo_ref, edge_ref, message_ref, p_ref, k_ref,
    p_edge, k_edge, slip_ref, basis_ref, sems,
):
    f32, bf16 = jnp.float32, jnp.bfloat16
    planes, rows = p_hbm.shape[0], p_hbm.shape[1]
    low = core_ref[0] != 0
    at = pl.multiple_of((1 - core_ref[0]) * (rows - 8), 8)
    parts = [pl.ds(i * (rows // 2), rows // 2) for i in range(2)]
    moves = [
        (source.at[planes - 1, part], target.at[part])
        for part in parts
        for source, target in ((p_hbm, p_ref), (k_hbm, k_ref))
    ]
    moves += [
        (p_hbm.at[:, pl.ds(at, 8)], p_edge),
        (k_hbm.at[:, pl.ds(at, 8)], k_edge),
        (slip_hbm, slip_ref),
        (basis_hbm, basis_ref),
    ]
    copies = [pltpu.make_async_copy(*move, sems.at[i]) for i, move in enumerate(moves)]
    for copy in copies:
        copy.start()
    for i, part in enumerate(parts):
        copies[2 * i].wait()
        halo_ref[0, part, :] = p_ref[part, :].astype(bf16)
        copies[2 * i + 1].wait()
        halo_ref[1, part, :] = k_ref[part, :].astype(f32).astype(bf16)
    for copy in copies[4:]:
        copy.wait()
    for plane in range(planes):
        block, kind = p_edge[plane], k_edge[plane].astype(f32)
        edge_ref[plane : plane + 1, :] = jnp.where(low, block[0:1, :], block[7:8, :])
        edge_ref[planes + plane : planes + plane + 1, :] = jnp.where(low, kind[0:1, :], kind[7:8, :])
    cells = slip_ref.shape[1]
    size = cells // clusters
    slip = slip_ref[...].astype(bf16).astype(f32)
    lines = [slip[:, at : at + 128] for at in range(0, size, 128)]
    lines += [slip[:, at : at + 128] for at in range(cells - size, cells, 128)]
    rank = basis_ref.shape[0]
    for cluster in range(clusters):
        part = slip[:, cluster * size : (cluster + 1) * size].astype(bf16)
        moment = lax.dot_general(
            jnp.broadcast_to(part, (16, size)),
            basis_ref[:, cluster * size : (cluster + 1) * size],
            (((1,), (1,)), ((), ())),
            preferred_element_type=f32,
        )[0:1, :]
        lines.append(jnp.concatenate([moment, jnp.zeros((1, 128 - rank), f32)], axis=1))
    height = message_ref.shape[1]
    lines.append(jnp.zeros((height - len(lines), 128), f32))
    message = jnp.concatenate(lines, axis=0).astype(bf16)
    for slab in range(message_ref.shape[0]):
        message_ref[slab] = message


def prepare(core, slab, pressure, region, slip, basis, clusters, slabs):
    planes, rows, width = pressure.shape
    cells = slip.shape[1]
    lines = 2 * (cells // clusters // 128) + clusters
    height = -(-lines // 16) * 16
    vmem, smem = pl.BlockSpec(memory_space=VMEM), pl.BlockSpec(memory_space=SMEM)
    return pl.pallas_call(
        functools.partial(prepare_kernel, clusters),
        in_specs=[smem] * 2 + [pl.BlockSpec(memory_space=pl.ANY)] * 4,
        out_specs=[vmem] * 3,
        out_shape=[
            VMEM_OUT((2, rows, width), jnp.bfloat16),
            VMEM_OUT((2 * planes, width), jnp.float32),
            VMEM_OUT((slabs, height, 128), jnp.bfloat16),
        ],
        scratch_shapes=[
            pltpu.VMEM((rows, width), pressure.dtype),
            pltpu.VMEM((rows, width), region.dtype),
            pltpu.VMEM((planes, 8, width), pressure.dtype),
            pltpu.VMEM((planes, 8, width), region.dtype),
            pltpu.VMEM(slip.shape, slip.dtype),
            pltpu.VMEM(basis.shape, basis.dtype),
            pltpu.SemaphoreType.DMA((8,)),
        ],
        name="prepare",
    )(core, slab, pressure, region, slip, basis)


def cells_kernel(
    core_ref, p_hbm, k_hbm, corner_ref, fraction_ref, slip_ref, leak_ref, sampled_ref, source_ref, p_ref, k_ref,
    field, sems, *slots, block
):
    _, rows, width = p_ref.shape
    f32, bf16, i16 = jnp.float32, jnp.bfloat16, jnp.int16
    steps = corner_ref.shape[1] // block
    iota = lax.broadcasted_iota(jnp.int32, (16, block), 0).astype(i16)
    iota_y = lax.broadcasted_iota(jnp.int32, (rows, block), 0)
    zero = jnp.float32(0.0)
    zeros = jnp.zeros((16, block), bf16)
    p_copy = pltpu.make_async_copy(p_hbm, p_ref, sems.at[0])
    k_copy = pltpu.make_async_copy(k_hbm, k_ref, sems.at[1])
    p_copy.start()

    def spread_rows(x, kind):
        return jnp.broadcast_to(x, (16, block)).astype(kind)

    def build(step, z_hi, z_lo, weight, scaled):
        at = slice(step * block, (step + 1) * block)
        frac_x, frac_y, frac_z = (fraction_ref[i : i + 1, at] for i in range(3))
        at_y = corner_ref[1:2, at] - core_ref[0] * rows
        at_z = spread_rows(corner_ref[2:3, at], i16)
        next_z = at_z + jnp.int16(1)
        low_z = 1.0 - frac_z
        low_hi, high_hi = spread_rows(low_z, bf16), spread_rows(frac_z, bf16)
        low_lo = (low_z - low_hi.astype(f32)).astype(bf16)
        high_lo = (frac_z - high_hi.astype(f32)).astype(bf16)
        for row in range(0, width, 16):
            here = iota == at_z - jnp.int16(row)
            above = iota == next_z - jnp.int16(row)
            z_hi[row : row + 16, :] = jnp.where(here, low_hi, jnp.where(above, high_hi, zeros))
            z_lo[row : row + 16, :] = jnp.where(here, low_lo, jnp.where(above, high_lo, zeros))
        weight_y = jnp.where(
            iota_y == at_y, 1.0 - frac_y, jnp.where(iota_y == at_y + 1, frac_y, zero)
        )
        weight[...] = weight_y
        flow = slip_ref[:, at] * leak_ref[:, at]
        for plane in range(2):
            weight_x = frac_x if plane else 1.0 - frac_x
            scaled[plane] = (weight_y * (weight_x * flow)).astype(bf16)

    def apply(step, z_hi, z_lo, weight, scaled):
        at = slice(step * block, (step + 1) * block)
        frac_x = fraction_ref[0:1, at]
        total = jnp.zeros((1, block), f32)
        for plane in range(2):
            weight_x = frac_x if plane else 1.0 - frac_x
            along = jnp.dot(field[plane], z_hi[...], preferred_element_type=f32)
            total = total + weight_x * jnp.sum(weight[...] * along, axis=0, keepdims=True)
            dims = (((1,), (1,)), ((), ()))
            spread = lax.dot_general(scaled[plane], z_hi[...], dims, preferred_element_type=f32)
            spread = spread + lax.dot_general(scaled[plane], z_lo[...], dims, preferred_element_type=f32)
            source_ref[plane] = spread if step == 0 else source_ref[plane] + spread
        sampled_ref[:, at] = total

    half = len(slots) // 2
    pair = (slots[:half], slots[half:])
    build(0, *pair[0])
    build(1, *pair[1])
    p_copy.wait()
    k_copy.start()
    field[...] = p_ref[...].astype(bf16)
    for step in range(steps):
        apply(step, *pair[step % 2])
        if step + 2 < steps:
            build(step + 2, *pair[step % 2])
    k_copy.wait()


def cells(core, pressure, region, corner, fraction, slip, leak, block):
    planes, rows, width = pressure.shape
    count = corner.shape[1]
    vmem, smem = pl.BlockSpec(memory_space=VMEM), pl.BlockSpec(memory_space=SMEM)
    hbm = pl.BlockSpec(memory_space=pl.ANY)
    slot = [
        pltpu.VMEM((width, block), jnp.bfloat16),
        pltpu.VMEM((width, block), jnp.bfloat16),
        pltpu.VMEM((rows, block), jnp.float32),
        pltpu.VMEM((planes, rows, block), jnp.bfloat16),
    ]
    return pl.pallas_call(
        functools.partial(cells_kernel, block=block),
        in_specs=[smem, hbm, hbm] + [vmem] * 4,
        out_specs=[vmem] * 4,
        out_shape=[
            VMEM_OUT((1, count), jnp.float32),
            VMEM_OUT(pressure.shape, jnp.float32),
            VMEM_OUT(pressure.shape, pressure.dtype),
            VMEM_OUT(region.shape, region.dtype),
        ],
        scratch_shapes=[pltpu.VMEM(pressure.shape, jnp.bfloat16), pltpu.SemaphoreType.DMA((2,))] + slot + slot,
        compiler_params=params(20),
        cost_estimate=pl.CostEstimate(
            flops=6 * planes * rows * width * count, bytes_accessed=8 * pressure.size, transcendentals=0
        ),
        name="cells",
    )(core, in_hbm(pressure), in_hbm(region), corner, fraction, slip, leak)


def stencil_kernel(
    core_ref, perm_ref, p_ref, k_ref, edge_ref, source_ref, out_ref, pad_p, pad_r
):
    planes, rows, width = p_ref.shape
    f32 = jnp.float32
    far = jnp.float32(jnp.inf)
    core = core_ref[0]
    table = make_table(perm_ref)
    outside = jnp.full((8, width), far, f32)
    for plane in range(planes):
        edge_p = jnp.broadcast_to(edge_ref[plane : plane + 1, :], (8, width))
        edge_k = edge_ref[planes + plane : planes + plane + 1, :].astype(jnp.int32)
        edge_r = lookup(table, jnp.broadcast_to(edge_k, (8, width)))
        pad_p[plane, 0:8, :] = edge_p
        pad_p[plane, rows + 8 : rows + 16, :] = edge_p
        pad_r[plane, 0:8, :] = jnp.where(core == 0, outside, edge_r)
        pad_r[plane, rows + 8 : rows + 16, :] = jnp.where(core == 0, edge_r, outside)

    def fill(s, carry):
        at = pl.multiple_of(s * 32, 8)
        to = pl.multiple_of(s * 32 + 8, 8)
        for plane in range(planes):
            pad_p[plane, pl.ds(to, 32), :] = p_ref[plane, pl.ds(at, 32), :]
            pad_r[plane, pl.ds(to, 32), :] = lookup(table, k_ref[plane, pl.ds(at, 32), :])
        return carry

    lax.fori_loop(0, rows // 32, fill, 0)
    lane = lax.broadcasted_iota(jnp.int32, (8, width), 1)
    sub = lax.broadcasted_iota(jnp.int32, (8, width), 0)

    def face(p, r, p_next, r_next):
        return 2.0 / (r + r_next) * (p_next - p)

    def y_face(plane, at):
        p, r = pad_p[plane, pl.ds(at, 8), :], pad_r[plane, pl.ds(at, 8), :]
        after = pl.multiple_of(at + 8, 8)
        pn, rn = pad_p[plane, pl.ds(after, 8), :], pad_r[plane, pl.ds(after, 8), :]
        pn = pltpu.roll(jnp.where(sub == 0, pn, p), 7, 0)
        rn = pltpu.roll(jnp.where(sub == 0, rn, r), 7, 0)
        return p, r, face(p, r, pn, rn)

    def strip(to, carry):
        at = pl.multiple_of(to + 8, 8)
        after = []
        sums, ps, rs = [], [], []
        for plane in range(planes):
            p, r, fy = y_face(plane, at)
            below = pltpu.roll(jnp.where(sub == 7, carry[plane], fy), 1, 0)
            after.append(fy)
            pz = pltpu.roll(p, width - 1, 1)
            rz = jnp.where(lane == width - 1, far, pltpu.roll(r, width - 1, 1))
            fz = face(p, r, pz, rz)
            sums.append(fy - below + (fz - pltpu.roll(fz, 1, 1)))
            ps.append(p)
            rs.append(r)
        for plane in range(planes - 1):
            fx = face(ps[plane], rs[plane], ps[plane + 1], rs[plane + 1])
            sums[plane] = sums[plane] + fx
            sums[plane + 1] = sums[plane + 1] - fx
        for plane in range(planes):
            out_ref[plane, pl.ds(to, 8), :] = source_ref[plane, pl.ds(to, 8), :] + sums[plane]
        return tuple(after)

    def body(s, carry):
        for at in range(0, UNROLL, 8):
            carry = strip(pl.multiple_of(s * UNROLL + at, 8), carry)
        return carry

    first = tuple(y_face(plane, 0)[2] for plane in range(planes))
    lax.fori_loop(0, rows // UNROLL, body, first)


def local_stencil(core, perm, pressure, region, edge, source):
    planes, rows, width = pressure.shape
    vmem, smem = pl.BlockSpec(memory_space=VMEM), pl.BlockSpec(memory_space=SMEM)
    return pl.pallas_call(
        stencil_kernel,
        in_specs=[smem, smem] + [vmem] * 4,
        out_specs=vmem,
        out_shape=VMEM_OUT(pressure.shape, jnp.float32),
        scratch_shapes=[pltpu.VMEM((planes, rows + 16, width), jnp.float32)] * 2,
        input_output_aliases={5: 0},
        compiler_params=params(20),
        cost_estimate=pl.CostEstimate(
            flops=200 * pressure.size, bytes_accessed=16 * pressure.size, transcendentals=0
        ),
        name="stencil",
    )(core, perm, pressure, region, edge, source)


def face_kernel(start, slab_ref, perm_ref, halo_ref, p_ref, region_ref, out_ref):
    valid = slab_ref[0] > 0
    far = jnp.float32(jnp.inf)
    table = make_table(perm_ref)

    def body(s, carry):
        at = pl.multiple_of(s * 32, 32)
        rows, own = pl.ds(at, 32), pl.ds(pl.multiple_of(start + at, 32), 32)
        other_p = halo_ref[0, own, :].astype(jnp.float32)
        other_r = lookup(table, halo_ref[1, own, :].astype(jnp.float32).astype(jnp.int32))
        other_r = jnp.where(valid, other_r, far)
        r = lookup(table, region_ref[0, own, :])
        flux = 2.0 / (r + other_r) * (other_p - p_ref[0, own, :])
        out_ref[rows, :] = flux.astype(jnp.bfloat16)
        return carry

    lax.fori_loop(0, out_ref.shape[0] // 32, body, 0)


def face_flux(slab, perm, halo, pressure, region, start, size):
    vmem, smem = pl.BlockSpec(memory_space=VMEM), pl.BlockSpec(memory_space=SMEM)
    return pl.pallas_call(
        functools.partial(face_kernel, start),
        in_specs=[smem, smem] + [vmem] * 3,
        out_specs=vmem,
        out_shape=VMEM_OUT((size, halo.shape[2]), jnp.bfloat16),
        compiler_params=params(8),
        name="face",
    )(slab, perm, halo, pressure, region)


def finish_kernel(
    acc_ref, mine_ref, theirs_ref, slip_ref, state_ref, a_ref, b_ref, normal_ref, *rest
):
    *highs, _, out_ref, accel_ref, rate_ref, final, sems = rest
    plane, rows = acc_ref.shape[0] - 1, acc_ref.shape[1]
    copies = []
    for i, (start, size) in enumerate(row_parts(rows)):
        part = pl.ds(start, size)
        final[part, :] = acc_ref[plane, part, :] - highs[i][...].astype(jnp.float32)
        copy = pltpu.make_async_copy(final.at[part], out_ref.at[plane, part], sems.at[i])
        copy.start()
        copies.append(copy)
    shares = mine_ref[...] + theirs_ref[...]
    slip = slip_ref[...]
    effective = normal_ref[...] - shares[1:2, :]
    change = jnp.exp(-state_ref[...]) - slip
    accel_ref[...] = (shares[0:1, :] - effective * b_ref[...] * change) / (
        effective * a_ref[...] / slip + 0.5
    )
    rate_ref[...] = change
    for copy in copies:
        copy.wait()


def finish(acc, *cell_args, highs, rate):
    count = cell_args[-1].shape[1]
    vmem, hbm = pl.BlockSpec(memory_space=VMEM), pl.BlockSpec(memory_space=pl.ANY)
    line = jax.ShapeDtypeStruct((1, count), jnp.float32)
    return pl.pallas_call(
        finish_kernel,
        in_specs=[vmem] * (8 + len(highs)) + [hbm],
        out_specs=[hbm, vmem, vmem],
        out_shape=[jax.ShapeDtypeStruct(acc.shape, jnp.float32), line, line],
        scratch_shapes=[pltpu.VMEM(acc.shape[1:], jnp.float32), pltpu.SemaphoreType.DMA((len(highs),))],
        input_output_aliases={8 + len(highs): 0},
        compiler_params=params(8),
        name="finish",
    )(acc, *cell_args, *highs, rate)


def traction_kernel(
    core_ref, slab_ref, got_ref, sampled_ref, slip_ref, near_hbm, coupling_hbm, row_ref, col_ref, rank_ref, basis_hbm,
    acc_ref, *rest, half_rows
):
    lows = rest[:-8]
    out_ref, rate_hbm, near_ref, coupling_ref, basis_ref, final, sems, final_sems = rest[-8:]
    moves = ((coupling_hbm, coupling_ref), (basis_hbm, basis_ref), (near_hbm, near_ref))
    coupling_copy, basis_copy, near_copy = (
        pltpu.make_async_copy(*move, sems.at[i]) for i, move in enumerate(moves)
    )
    coupling_copy.start()
    basis_copy.start()
    near_copy.start()
    final_copies = []
    for i, (start, size) in enumerate(row_parts(acc_ref.shape[1])):
        part = pl.ds(start, size)
        final[part, :] = acc_ref[0, part, :] + lows[i][...].astype(jnp.float32)
        copy = pltpu.make_async_copy(final.at[part], rate_hbm.at[0, part], final_sems.at[i])
        copy.start()
        final_copies.append(copy)
    f32, bf16 = jnp.float32, jnp.bfloat16
    core, slab = core_ref[0], slab_ref[0]
    slabs = got_ref.shape[0]
    rank, cells = basis_ref.shape
    size = near_ref.shape[2]
    clusters = cells // size
    per = size // 128
    slots = row_ref.shape[1]

    cols, rows, ranks = col_ref[...], row_ref[...], rank_ref[...]
    owner, member = cols // clusters, cols % clusters
    slab_iota = lax.broadcasted_iota(jnp.int32, (slabs, slots), 0)
    pick = (slab_iota == owner).astype(f32).astype(bf16)
    picked = jnp.zeros((128, slots), f32)
    for cluster in range(clusters):
        sent = got_ref[:, 2 * per + cluster, :]
        chosen = lax.dot_general(sent, pick, (((0,), (0,)), ((), ())), preferred_element_type=f32)
        picked = jnp.where(member == cluster, chosen, picked)
    rank_iota = lax.broadcasted_iota(jnp.int32, (rank, slots), 0)
    masked = jnp.where(rank_iota < ranks, picked[:rank, :], jnp.float32(0.0))
    coupling_copy.wait()
    lines = []
    for a in range(rank):
        lines.append(jnp.sum(coupling_ref[a].astype(f32) * masked, axis=0, keepdims=True))
    block = jnp.concatenate(lines, axis=0)
    basis_copy.wait()
    far = []
    for cluster in range(clusters):
        total = jnp.sum(jnp.where(rows == cluster, block, jnp.float32(0.0)), axis=1, keepdims=True)
        basis = basis_ref[:, cluster * size : (cluster + 1) * size].astype(f32)
        far.append(jnp.sum(basis * total, axis=0, keepdims=True))

    def line(slab_at, row):
        parts = [got_ref[pl.ds(slab_at, 1), row + i, :].astype(f32) for i in range(per)]
        return jnp.concatenate(parts, axis=1)

    zero = jnp.zeros((1, size), f32)
    before = jnp.where(slab > 0, line(jnp.maximum(slab - 1, 0), per), zero)
    after = jnp.where(slab < slabs - 1, line(jnp.minimum(slab + 1, slabs - 1), 0), zero)
    slip = slip_ref[...].astype(bf16).astype(f32)
    extended = [before] + [slip[:, c * size : (c + 1) * size] for c in range(clusters)] + [after]
    near_copy.wait()
    near = []
    for i in range(half_rows):
        total = jnp.zeros((16, size), f32)
        for j in range(3):
            source = jnp.where(core == 0, extended[i + j], extended[half_rows + i + j])
            total = total + lax.dot_general(
                jnp.broadcast_to(source, (16, size)).astype(bf16),
                near_ref[i, j],
                (((1,), (1,)), ((), ())),
                preferred_element_type=f32,
            )
        near.append(total[0:1, :])
    for cluster in range(clusters):
        mine = (cluster // half_rows) == core
        out_ref[0:1, cluster * size : (cluster + 1) * size] = far[cluster] + jnp.where(
            mine, near[cluster % half_rows], zero
        )
    out_ref[1:2, :] = sampled_ref[...]
    for copy in final_copies:
        copy.wait()


def traction_share(core, slab, got, sampled, slip, near_blocks, coupling, rows, cols, ranks, basis, acc, lows):
    vmem, smem = pl.BlockSpec(memory_space=VMEM), pl.BlockSpec(memory_space=SMEM)
    hbm = pl.BlockSpec(memory_space=pl.ANY)
    return pl.pallas_call(
        functools.partial(traction_kernel, half_rows=near_blocks.shape[0]),
        in_specs=[smem] * 2 + [vmem] * 3 + [hbm] * 2 + [vmem] * 3 + [hbm] + [vmem] * (1 + len(lows)),
        out_specs=[vmem, hbm],
        out_shape=[
            VMEM_OUT((2, slip.shape[1]), jnp.float32),
            jax.ShapeDtypeStruct(acc.shape, jnp.float32),
        ],
        scratch_shapes=[
            pltpu.VMEM(near_blocks.shape, near_blocks.dtype),
            pltpu.VMEM(coupling.shape, coupling.dtype),
            pltpu.VMEM(basis.shape, basis.dtype),
            pltpu.VMEM(acc.shape[1:], acc.dtype),
            pltpu.SemaphoreType.DMA((3,)),
            pltpu.SemaphoreType.DMA((len(lows),)),
        ],
        compiler_params=params(16),
        name="traction",
    )(
        core, slab, got, sampled, slip, in_hbm(near_blocks), in_hbm(coupling), rows, cols, ranks, in_hbm(basis),
        acc, *lows,
    )


def shards(
    slip_rate,
    log_state,
    friction_a,
    friction_b,
    normal_stress,
    leak_rate,
    corner,
    fraction,
    near_blocks,
    row_basis,
    col_basis,
    far_row,
    far_col,
    far_rank,
    far_coupling,
    pressure,
    region,
    perm_table,
):
    slab = lax.axis_index("slab").astype(jnp.int32)
    core = lax.axis_index("blk").astype(jnp.int32)
    slabs = lax.axis_size("slab")
    _, rows, _ = pressure.shape
    cluster_size = near_blocks.shape[2]
    fault_cells = slip_rate.shape[0]
    clusters = fault_cells // cluster_size
    forward = [(i, i + 1) for i in range(slabs - 1)]
    backward = [(target, source) for source, target in forward]
    swap = [(0, 1), (1, 0)]
    core, slab = core.reshape(1), slab.reshape(1)
    line = lambda x: x.reshape(1, -1)
    slip = line(slip_rate)
    p_in, k_in = in_hbm(pressure), in_hbm(region)

    halo, edge, message = prepare(
        core, slab, p_in, k_in, in_hbm(slip), in_hbm(col_basis), clusters, slabs
    )
    halo = lax.ppermute(halo, "slab", forward)
    got = lax.all_to_all(message, "slab", 0, 0, tiled=True)
    edge = lax.ppermute(edge, "blk", swap)

    sampled, source, p, k = cells(
        core, pressure, region, corner, fraction, slip, line(leak_rate), 512
    )
    acc = local_stencil(core, perm_table, p, k, edge, source)
    lows, highs = [], []
    for start, size in row_parts(rows):
        low = face_flux(slab, perm_table, halo, p, k, start, size)
        highs.append(lax.ppermute(low, "slab", backward))
        lows.append(low)

    got, acc = lax.optimization_barrier((got, acc, *lows))[:2]
    shares, rate = traction_share(
        core,
        slab,
        got,
        sampled,
        slip,
        near_blocks,
        far_coupling,
        line(far_row),
        line(far_col),
        line(far_rank),
        row_basis,
        acc,
        lows,
    )
    others = lax.ppermute(shares, "blk", swap)
    rate, accel, change = finish(
        acc,
        shares,
        others,
        slip,
        line(log_state),
        line(friction_a),
        line(friction_b),
        line(normal_stress),
        highs=highs,
        rate=rate,
    )
    return (accel.reshape(-1), change.reshape(-1), rate)


def solution(mesh):
    placed = (
        P("slab"),
        P("slab"),
        P("slab"),
        P("slab"),
        P("slab"),
        P("slab"),
        P(None, "slab"),
        P(None, "slab"),
        P(("slab", "blk"), None, None, None),
        P(None, "slab"),
        P(None, "slab"),
        P(("slab", "blk")),
        P(("slab", "blk")),
        P(("slab", "blk")),
        P(None, None, ("slab", "blk")),
        P("slab", "blk", None),
        P("slab", "blk", None),
        P(),
    )

    return jax.shard_map(
        shards,
        mesh=mesh,
        in_specs=placed,
        out_specs=(P("slab"), P("slab"), P("slab", "blk", None)),
        check_vma=False,
    )
```

```python
import functools

import jax
import jax.numpy as jnp
from jax import lax
from jax.experimental import pallas as pl
from jax.experimental.pallas import tpu as pltpu
from jax.sharding import PartitionSpec as P


VMEM = pltpu.MemorySpace.VMEM
SMEM = pltpu.MemorySpace.SMEM
UNROLL = 16
PARTS = (5, 3)
VMEM_OUT = pltpu.VMEM


def row_parts(rows):
    sizes = [rows * part // sum(PARTS) for part in PARTS]
    return [(sum(sizes[:i]), size) for i, size in enumerate(sizes)]


def params(megabytes):
    return pltpu.CompilerParams(vmem_limit_bytes=megabytes << 20)


def in_hbm(x):
    return pltpu.with_memory_space_constraint(x, pltpu.MemorySpace.HBM)


def make_table(values_ref):
    lane = lax.broadcasted_iota(jnp.int32, (8, 128), 1)
    table = jnp.ones((8, 128), jnp.float32)
    for i in range(values_ref.shape[0]):
        table = jnp.where(lane == i, values_ref[i], table)
    return 1.0 / table


def lookup(table, index):
    height, width = index.shape
    table = jnp.concatenate([table] * (height // 8), axis=0)
    parts = [
        jnp.take_along_axis(table, index[:, at : at + 128], axis=1) for at in range(0, width, 128)
    ]
    return jnp.concatenate(parts, axis=1)


def prepare_kernel(
    clusters, core_ref, slab_ref, p_hbm, k_hbm, slip_hbm, basis_hbm, *rest
):
    *halo_refs, edge_ref, message_ref, p_ref, k_ref, p_edge, k_edge, slip_ref, basis_ref, sems = rest
    f32, bf16 = jnp.float32, jnp.bfloat16
    planes, rows = p_hbm.shape[0], p_hbm.shape[1]
    low = core_ref[0] != 0
    at = pl.multiple_of((1 - core_ref[0]) * (rows - 8), 8)
    parts = [pl.ds(start, size) for start, size in row_parts(rows)]
    moves = [
        (source.at[planes - 1, part], target.at[part])
        for part in parts
        for source, target in ((p_hbm, p_ref), (k_hbm, k_ref))
    ]
    moves += [
        (p_hbm.at[:, pl.ds(at, 8)], p_edge),
        (k_hbm.at[:, pl.ds(at, 8)], k_edge),
        (slip_hbm, slip_ref),
        (basis_hbm, basis_ref),
    ]
    copies = [pltpu.make_async_copy(*move, sems.at[i]) for i, move in enumerate(moves)]
    for copy in copies:
        copy.start()
    for i, part in enumerate(parts):
        copies[2 * i].wait()
        halo_refs[i][0] = p_ref[part, :].astype(bf16)
        copies[2 * i + 1].wait()
        halo_refs[i][1] = k_ref[part, :].astype(f32).astype(bf16)
    for copy in copies[2 * len(parts) :]:
        copy.wait()
    for plane in range(planes):
        block, kind = p_edge[plane], k_edge[plane].astype(f32)
        edge_ref[plane : plane + 1, :] = jnp.where(low, block[0:1, :], block[7:8, :])
        edge_ref[planes + plane : planes + plane + 1, :] = jnp.where(low, kind[0:1, :], kind[7:8, :])
    cells = slip_ref.shape[1]
    size = cells // clusters
    slip = slip_ref[...].astype(bf16).astype(f32)
    lines = [slip[:, at : at + 128] for at in range(0, size, 128)]
    lines += [slip[:, at : at + 128] for at in range(cells - size, cells, 128)]
    rank = basis_ref.shape[0]
    for cluster in range(clusters):
        part = slip[:, cluster * size : (cluster + 1) * size].astype(bf16)
        moment = lax.dot_general(
            jnp.broadcast_to(part, (16, size)),
            basis_ref[:, cluster * size : (cluster + 1) * size],
            (((1,), (1,)), ((), ())),
            preferred_element_type=f32,
        )[0:1, :]
        lines.append(jnp.concatenate([moment, jnp.zeros((1, 128 - rank), f32)], axis=1))
    height = message_ref.shape[1]
    lines.append(jnp.zeros((height - len(lines), 128), f32))
    message = jnp.concatenate(lines, axis=0).astype(bf16)
    for slab in range(message_ref.shape[0]):
        message_ref[slab] = message


def prepare(core, slab, pressure, region, slip, basis, clusters, slabs):
    planes, rows, width = pressure.shape
    cells = slip.shape[1]
    lines = 2 * (cells // clusters // 128) + clusters
    height = -(-lines // 16) * 16
    vmem, smem = pl.BlockSpec(memory_space=VMEM), pl.BlockSpec(memory_space=SMEM)
    return pl.pallas_call(
        functools.partial(prepare_kernel, clusters),
        in_specs=[smem] * 2 + [pl.BlockSpec(memory_space=pl.ANY)] * 4,
        out_specs=[vmem] * (2 + len(PARTS)),
        out_shape=[VMEM_OUT((2, size, width), jnp.bfloat16) for _, size in row_parts(rows)]
        + [
            VMEM_OUT((2 * planes, width), jnp.float32),
            VMEM_OUT((slabs, height, 128), jnp.bfloat16),
        ],
        scratch_shapes=[
            pltpu.VMEM((rows, width), pressure.dtype),
            pltpu.VMEM((rows, width), region.dtype),
            pltpu.VMEM((planes, 8, width), pressure.dtype),
            pltpu.VMEM((planes, 8, width), region.dtype),
            pltpu.VMEM(slip.shape, slip.dtype),
            pltpu.VMEM(basis.shape, basis.dtype),
            pltpu.SemaphoreType.DMA((4 + 2 * len(PARTS),)),
        ],
        name="prepare",
    )(core, slab, pressure, region, slip, basis)


def cells_kernel(
    core_ref, p_hbm, k_hbm, corner_ref, fraction_ref, slip_ref, leak_ref, sampled_ref, source_ref, p_ref, k_ref,
    field, sems, *slots, block
):
    _, rows, width = p_ref.shape
    f32, bf16, i16 = jnp.float32, jnp.bfloat16, jnp.int16
    steps = corner_ref.shape[1] // block
    iota = lax.broadcasted_iota(jnp.int32, (16, block), 0).astype(i16)
    iota_y = lax.broadcasted_iota(jnp.int32, (rows, block), 0)
    zero = jnp.float32(0.0)
    zeros = jnp.zeros((16, block), bf16)
    p_copy = pltpu.make_async_copy(p_hbm, p_ref, sems.at[0])
    k_copy = pltpu.make_async_copy(k_hbm, k_ref, sems.at[1])
    p_copy.start()

    def spread_rows(x, kind):
        return jnp.broadcast_to(x, (16, block)).astype(kind)

    def build(step, z_hi, z_lo, weight, scaled):
        at = slice(step * block, (step + 1) * block)
        frac_x, frac_y, frac_z = (fraction_ref[i : i + 1, at] for i in range(3))
        at_y = corner_ref[1:2, at] - core_ref[0] * rows
        at_z = spread_rows(corner_ref[2:3, at], i16)
        next_z = at_z + jnp.int16(1)
        low_z = 1.0 - frac_z
        low_hi, high_hi = spread_rows(low_z, bf16), spread_rows(frac_z, bf16)
        low_lo = (low_z - low_hi.astype(f32)).astype(bf16)
        high_lo = (frac_z - high_hi.astype(f32)).astype(bf16)
        for row in range(0, width, 16):
            here = iota == at_z - jnp.int16(row)
            above = iota == next_z - jnp.int16(row)
            z_hi[row : row + 16, :] = jnp.where(here, low_hi, jnp.where(above, high_hi, zeros))
            z_lo[row : row + 16, :] = jnp.where(here, low_lo, jnp.where(above, high_lo, zeros))
        weight_y = jnp.where(
            iota_y == at_y, 1.0 - frac_y, jnp.where(iota_y == at_y + 1, frac_y, zero)
        )
        weight[...] = weight_y
        flow = slip_ref[:, at] * leak_ref[:, at]
        for plane in range(2):
            weight_x = frac_x if plane else 1.0 - frac_x
            scaled[plane] = (weight_y * (weight_x * flow)).astype(bf16)

    def apply(step, z_hi, z_lo, weight, scaled):
        at = slice(step * block, (step + 1) * block)
        frac_x = fraction_ref[0:1, at]
        total = jnp.zeros((1, block), f32)
        for plane in range(2):
            weight_x = frac_x if plane else 1.0 - frac_x
            along = jnp.dot(field[plane], z_hi[...], preferred_element_type=f32)
            total = total + weight_x * jnp.sum(weight[...] * along, axis=0, keepdims=True)
            dims = (((1,), (1,)), ((), ()))
            spread = lax.dot_general(scaled[plane], z_hi[...], dims, preferred_element_type=f32)
            spread = spread + lax.dot_general(scaled[plane], z_lo[...], dims, preferred_element_type=f32)
            source_ref[plane] = spread if step == 0 else source_ref[plane] + spread
        sampled_ref[:, at] = total

    half = len(slots) // 2
    pair = (slots[:half], slots[half:])
    build(0, *pair[0])
    build(1, *pair[1])
    p_copy.wait()
    k_copy.start()
    field[...] = p_ref[...].astype(bf16)
    for step in range(steps):
        apply(step, *pair[step % 2])
        if step + 2 < steps:
            build(step + 2, *pair[step % 2])
    k_copy.wait()


def cells(core, pressure, region, corner, fraction, slip, leak, block):
    planes, rows, width = pressure.shape
    count = corner.shape[1]
    vmem, smem = pl.BlockSpec(memory_space=VMEM), pl.BlockSpec(memory_space=SMEM)
    hbm = pl.BlockSpec(memory_space=pl.ANY)
    slot = [
        pltpu.VMEM((width, block), jnp.bfloat16),
        pltpu.VMEM((width, block), jnp.bfloat16),
        pltpu.VMEM((rows, block), jnp.float32),
        pltpu.VMEM((planes, rows, block), jnp.bfloat16),
    ]
    return pl.pallas_call(
        functools.partial(cells_kernel, block=block),
        in_specs=[smem, hbm, hbm] + [vmem] * 4,
        out_specs=[vmem] * 4,
        out_shape=[
            VMEM_OUT((1, count), jnp.float32),
            VMEM_OUT(pressure.shape, jnp.float32),
            VMEM_OUT(pressure.shape, pressure.dtype),
            VMEM_OUT(region.shape, region.dtype),
        ],
        scratch_shapes=[pltpu.VMEM(pressure.shape, jnp.bfloat16), pltpu.SemaphoreType.DMA((2,))] + slot + slot,
        compiler_params=params(20),
        cost_estimate=pl.CostEstimate(
            flops=6 * planes * rows * width * count, bytes_accessed=8 * pressure.size, transcendentals=0
        ),
        name="cells",
    )(core, in_hbm(pressure), in_hbm(region), corner, fraction, slip, leak)


def stencil_kernel(
    core_ref, perm_ref, p_ref, k_ref, edge_ref, source_ref, low_ref, rate_hbm, last_ref, rest_ref, pad_p, pad_r,
    final, sems,
):
    planes, rows, width = p_ref.shape
    f32 = jnp.float32
    far = jnp.float32(jnp.inf)
    core = core_ref[0]
    table = make_table(perm_ref)
    outside = jnp.full((8, width), far, f32)
    for plane in range(planes):
        edge_p = jnp.broadcast_to(edge_ref[plane : plane + 1, :], (8, width))
        edge_k = edge_ref[planes + plane : planes + plane + 1, :].astype(jnp.int32)
        edge_r = lookup(table, jnp.broadcast_to(edge_k, (8, width)))
        pad_p[plane, 0:8, :] = edge_p
        pad_p[plane, rows + 8 : rows + 16, :] = edge_p
        pad_r[plane, 0:8, :] = jnp.where(core == 0, outside, edge_r)
        pad_r[plane, rows + 8 : rows + 16, :] = jnp.where(core == 0, edge_r, outside)

    def fill(s, carry):
        at = pl.multiple_of(s * 32, 8)
        to = pl.multiple_of(s * 32 + 8, 8)
        for plane in range(planes):
            pad_p[plane, pl.ds(to, 32), :] = p_ref[plane, pl.ds(at, 32), :]
            pad_r[plane, pl.ds(to, 32), :] = lookup(table, k_ref[plane, pl.ds(at, 32), :])
        return carry

    lax.fori_loop(0, rows // 32, fill, 0)
    lane = lax.broadcasted_iota(jnp.int32, (8, width), 1)
    sub = lax.broadcasted_iota(jnp.int32, (8, width), 0)

    def face(p, r, p_next, r_next):
        return 2.0 / (r + r_next) * (p_next - p)

    def y_face(plane, at):
        p, r = pad_p[plane, pl.ds(at, 8), :], pad_r[plane, pl.ds(at, 8), :]
        after = pl.multiple_of(at + 8, 8)
        pn, rn = pad_p[plane, pl.ds(after, 8), :], pad_r[plane, pl.ds(after, 8), :]
        pn = pltpu.roll(jnp.where(sub == 0, pn, p), 7, 0)
        rn = pltpu.roll(jnp.where(sub == 0, rn, r), 7, 0)
        return p, r, face(p, r, pn, rn)

    def strip(to, low, carry):
        at = pl.multiple_of(to + 8, 8)
        after = []
        sums, ps, rs = [], [], []
        for plane in range(planes):
            p, r, fy = y_face(plane, at)
            below = pltpu.roll(jnp.where(sub == 7, carry[plane], fy), 1, 0)
            after.append(fy)
            pz = pltpu.roll(p, width - 1, 1)
            rz = jnp.where(lane == width - 1, far, pltpu.roll(r, width - 1, 1))
            fz = face(p, r, pz, rz)
            sums.append(fy - below + (fz - pltpu.roll(fz, 1, 1)))
            ps.append(p)
            rs.append(r)
        for plane in range(planes - 1):
            fx = face(ps[plane], rs[plane], ps[plane + 1], rs[plane + 1])
            sums[plane] = sums[plane] + fx
            sums[plane + 1] = sums[plane + 1] - fx
        for plane in range(planes):
            sums[plane] = source_ref[plane, pl.ds(to, 8), :] + sums[plane]
        last_ref[pl.ds(to, 8), :] = sums[1]
        if low is None:
            rest_ref[pl.ds(to - final.shape[0], 8), :] = sums[0]
        else:
            final[pl.ds(to, 8), :] = sums[0] + low
        return tuple(after)

    def body(s, carry):
        rows_at = pl.multiple_of(s * UNROLL, UNROLL)
        low = low_ref[pl.ds(rows_at, UNROLL), :].astype(f32)
        for at in range(0, UNROLL, 8):
            carry = strip(pl.multiple_of(rows_at + at, 8), low[at : at + 8], carry)
        return carry

    def rest_body(s, carry):
        for at in range(0, UNROLL, 8):
            carry = strip(pl.multiple_of(s * UNROLL + at, 8), None, carry)
        return carry

    carry = tuple(y_face(plane, 0)[2] for plane in range(planes))
    done = final.shape[0]
    carry = lax.fori_loop(0, done // UNROLL, body, carry)
    copy = pltpu.make_async_copy(final, rate_hbm.at[0, pl.ds(0, done)], sems.at[0])
    copy.start()
    lax.fori_loop(done // UNROLL, rows // UNROLL, rest_body, carry)
    copy.wait()


def local_stencil(core, perm, pressure, region, edge, source, low):
    planes, rows, width = pressure.shape
    done = low.shape[0]
    vmem, smem = pl.BlockSpec(memory_space=VMEM), pl.BlockSpec(memory_space=SMEM)
    return pl.pallas_call(
        stencil_kernel,
        in_specs=[smem, smem] + [vmem] * 5,
        out_specs=[pl.BlockSpec(memory_space=pl.ANY), vmem, vmem],
        out_shape=[
            jax.ShapeDtypeStruct(pressure.shape, jnp.float32),
            VMEM_OUT((rows, width), jnp.float32),
            VMEM_OUT((rows - done, width), jnp.float32),
        ],
        scratch_shapes=[pltpu.VMEM((planes, rows + 16, width), jnp.float32)] * 2
        + [pltpu.VMEM((done, width), jnp.float32), pltpu.SemaphoreType.DMA((1,))],
        compiler_params=params(20),
        cost_estimate=pl.CostEstimate(
            flops=200 * pressure.size, bytes_accessed=16 * pressure.size, transcendentals=0
        ),
        name="stencil",
    )(core, perm, pressure, region, edge, source, low)


def face_kernel(start, slab_ref, perm_ref, halo_ref, p_ref, region_ref, out_ref):
    valid = slab_ref[0] > 0
    far = jnp.float32(jnp.inf)
    table = make_table(perm_ref)

    def body(s, carry):
        at = pl.multiple_of(s * 32, 32)
        rows, own = pl.ds(at, 32), pl.ds(pl.multiple_of(start + at, 32), 32)
        other_p = halo_ref[0, rows, :].astype(jnp.float32)
        other_r = lookup(table, halo_ref[1, rows, :].astype(jnp.float32).astype(jnp.int32))
        other_r = jnp.where(valid, other_r, far)
        r = lookup(table, region_ref[0, own, :])
        flux = 2.0 / (r + other_r) * (other_p - p_ref[0, own, :])
        out_ref[rows, :] = flux.astype(jnp.bfloat16)
        return carry

    lax.fori_loop(0, out_ref.shape[0] // 32, body, 0)


def face_flux(slab, perm, halo, pressure, region, start):
    vmem, smem = pl.BlockSpec(memory_space=VMEM), pl.BlockSpec(memory_space=SMEM)
    return pl.pallas_call(
        functools.partial(face_kernel, start),
        in_specs=[smem, smem] + [vmem] * 3,
        out_specs=vmem,
        out_shape=VMEM_OUT(halo.shape[1:], jnp.bfloat16),
        compiler_params=params(8),
        name="face",
    )(slab, perm, halo, pressure, region)


def finish_kernel(
    last_ref, rest_acc, mine_ref, theirs_ref, slip_ref, state_ref, a_ref, b_ref, normal_ref, *rest
):
    *fluxes, _, out_ref, accel_ref, rate_ref, final, rest_final, sems = rest
    rows = last_ref.shape[0]
    parts = row_parts(rows)
    lows, highs = fluxes[: len(parts) - 1], fluxes[len(parts) - 1 :]
    copies = []

    def send(source, target, sem):
        copy = pltpu.make_async_copy(source, target, sem)
        copy.start()
        copies.append(copy)

    for i, (start, size) in enumerate(parts):
        part = pl.ds(start, size)
        if i:
            here = pl.ds(start - parts[0][1], size)
            rest_final[here, :] = rest_acc[here, :] + lows[i - 1][...].astype(jnp.float32)
            send(rest_final.at[here], out_ref.at[0, part], sems.at[0, i])
        final[part, :] = last_ref[part, :] - highs[i][...].astype(jnp.float32)
        send(final.at[part], out_ref.at[1, part], sems.at[1, i])
    shares = mine_ref[...] + theirs_ref[...]
    slip = slip_ref[...]
    effective = normal_ref[...] - shares[1:2, :]
    change = jnp.exp(-state_ref[...]) - slip
    accel_ref[...] = (shares[0:1, :] - effective * b_ref[...] * change) / (
        effective * a_ref[...] / slip + 0.5
    )
    rate_ref[...] = change
    for copy in copies:
        copy.wait()


def finish(last, rest, *cell_args, fluxes, rate):
    count = cell_args[-1].shape[1]
    vmem, hbm = pl.BlockSpec(memory_space=VMEM), pl.BlockSpec(memory_space=pl.ANY)
    line = jax.ShapeDtypeStruct((1, count), jnp.float32)
    return pl.pallas_call(
        finish_kernel,
        in_specs=[vmem] * (9 + len(fluxes)) + [hbm],
        out_specs=[hbm, vmem, vmem],
        out_shape=[jax.ShapeDtypeStruct(rate.shape, jnp.float32), line, line],
        scratch_shapes=[
            pltpu.VMEM(last.shape, jnp.float32),
            pltpu.VMEM(rest.shape, jnp.float32),
            pltpu.SemaphoreType.DMA((2, len(PARTS))),
        ],
        input_output_aliases={9 + len(fluxes): 0},
        compiler_params=params(8),
        name="finish",
    )(last, rest, *cell_args, *fluxes, rate)


def traction_kernel(
    core_ref, slab_ref, got_ref, sampled_ref, slip_ref, near_hbm, coupling_hbm, row_ref, col_ref, rank_ref, basis_hbm,
    out_ref, near_ref, coupling_ref, basis_ref, sems, *, half_rows
):
    moves = ((coupling_hbm, coupling_ref), (basis_hbm, basis_ref), (near_hbm, near_ref))
    coupling_copy, basis_copy, near_copy = (
        pltpu.make_async_copy(*move, sems.at[i]) for i, move in enumerate(moves)
    )
    coupling_copy.start()
    basis_copy.start()
    near_copy.start()
    f32, bf16 = jnp.float32, jnp.bfloat16
    core, slab = core_ref[0], slab_ref[0]
    slabs = got_ref.shape[0]
    rank, cells = basis_ref.shape
    size = near_ref.shape[2]
    clusters = cells // size
    per = size // 128
    slots = row_ref.shape[1]

    cols, rows, ranks = col_ref[...], row_ref[...], rank_ref[...]
    owner, member = cols // clusters, cols % clusters
    slab_iota = lax.broadcasted_iota(jnp.int32, (slabs, slots), 0)
    pick = (slab_iota == owner).astype(f32).astype(bf16)
    picked = jnp.zeros((128, slots), f32)
    for cluster in range(clusters):
        sent = got_ref[:, 2 * per + cluster, :]
        chosen = lax.dot_general(sent, pick, (((0,), (0,)), ((), ())), preferred_element_type=f32)
        picked = jnp.where(member == cluster, chosen, picked)
    rank_iota = lax.broadcasted_iota(jnp.int32, (rank, slots), 0)
    masked = jnp.where(rank_iota < ranks, picked[:rank, :], jnp.float32(0.0))
    coupling_copy.wait()
    lines = []
    for a in range(rank):
        lines.append(jnp.sum(coupling_ref[a].astype(f32) * masked, axis=0, keepdims=True))
    block = jnp.concatenate(lines, axis=0)
    basis_copy.wait()
    far = []
    for cluster in range(clusters):
        total = jnp.sum(jnp.where(rows == cluster, block, jnp.float32(0.0)), axis=1, keepdims=True)
        basis = basis_ref[:, cluster * size : (cluster + 1) * size].astype(f32)
        far.append(jnp.sum(basis * total, axis=0, keepdims=True))

    def line(slab_at, row):
        parts = [got_ref[pl.ds(slab_at, 1), row + i, :].astype(f32) for i in range(per)]
        return jnp.concatenate(parts, axis=1)

    zero = jnp.zeros((1, size), f32)
    before = jnp.where(slab > 0, line(jnp.maximum(slab - 1, 0), per), zero)
    after = jnp.where(slab < slabs - 1, line(jnp.minimum(slab + 1, slabs - 1), 0), zero)
    slip = slip_ref[...].astype(bf16).astype(f32)
    extended = [before] + [slip[:, c * size : (c + 1) * size] for c in range(clusters)] + [after]
    near_copy.wait()
    near = []
    for i in range(half_rows):
        total = jnp.zeros((16, size), f32)
        for j in range(3):
            source = jnp.where(core == 0, extended[i + j], extended[half_rows + i + j])
            total = total + lax.dot_general(
                jnp.broadcast_to(source, (16, size)).astype(bf16),
                near_ref[i, j],
                (((1,), (1,)), ((), ())),
                preferred_element_type=f32,
            )
        near.append(total[0:1, :])
    for cluster in range(clusters):
        mine = (cluster // half_rows) == core
        out_ref[0:1, cluster * size : (cluster + 1) * size] = far[cluster] + jnp.where(
            mine, near[cluster % half_rows], zero
        )
    out_ref[1:2, :] = sampled_ref[...]


def traction_share(core, slab, got, sampled, slip, near_blocks, coupling, rows, cols, ranks, basis):
    vmem, smem = pl.BlockSpec(memory_space=VMEM), pl.BlockSpec(memory_space=SMEM)
    hbm = pl.BlockSpec(memory_space=pl.ANY)
    return pl.pallas_call(
        functools.partial(traction_kernel, half_rows=near_blocks.shape[0]),
        in_specs=[smem] * 2 + [vmem] * 3 + [hbm] * 2 + [vmem] * 3 + [hbm],
        out_specs=vmem,
        out_shape=VMEM_OUT((2, slip.shape[1]), jnp.float32),
        scratch_shapes=[
            pltpu.VMEM(near_blocks.shape, near_blocks.dtype),
            pltpu.VMEM(coupling.shape, coupling.dtype),
            pltpu.VMEM(basis.shape, basis.dtype),
            pltpu.SemaphoreType.DMA((3,)),
        ],
        compiler_params=params(16),
        name="traction",
    )(core, slab, got, sampled, slip, in_hbm(near_blocks), in_hbm(coupling), rows, cols, ranks, in_hbm(basis))


def shards(
    slip_rate,
    log_state,
    friction_a,
    friction_b,
    normal_stress,
    leak_rate,
    corner,
    fraction,
    near_blocks,
    row_basis,
    col_basis,
    far_row,
    far_col,
    far_rank,
    far_coupling,
    pressure,
    region,
    perm_table,
):
    slab = lax.axis_index("slab").astype(jnp.int32)
    core = lax.axis_index("blk").astype(jnp.int32)
    slabs = lax.axis_size("slab")
    _, rows, _ = pressure.shape
    cluster_size = near_blocks.shape[2]
    fault_cells = slip_rate.shape[0]
    clusters = fault_cells // cluster_size
    forward = [(i, i + 1) for i in range(slabs - 1)]
    backward = [(target, source) for source, target in forward]
    swap = [(0, 1), (1, 0)]
    core, slab = core.reshape(1), slab.reshape(1)
    line = lambda x: x.reshape(1, -1)
    slip = line(slip_rate)
    p_in, k_in = in_hbm(pressure), in_hbm(region)

    *halos, edge, message = prepare(
        core, slab, p_in, k_in, in_hbm(slip), in_hbm(col_basis), clusters, slabs
    )
    for i in range(len(halos)):
        halos[i] = lax.ppermute(halos[i], "slab", forward)
    got = lax.all_to_all(message, "slab", 0, 0, tiled=True)
    edge = lax.ppermute(edge, "blk", swap)

    sampled, source, p, k = cells(
        core, pressure, region, corner, fraction, slip, line(leak_rate), 512
    )
    lows, highs = [], []
    for i, (start, size) in enumerate(row_parts(rows)):
        low = face_flux(slab, perm_table, halos[i], p, k, start)
        highs.append(lax.ppermute(low, "slab", backward))
        lows.append(low)
        if i == 0:
            rate, last, rest = local_stencil(core, perm_table, p, k, edge, source, low)

    got, last = lax.optimization_barrier((got, last, lows[-1]))[:2]
    shares = traction_share(
        core,
        slab,
        got,
        sampled,
        slip,
        near_blocks,
        far_coupling,
        line(far_row),
        line(far_col),
        line(far_rank),
        row_basis,
    )
    others = lax.ppermute(shares, "blk", swap)
    rate, accel, change = finish(
        last,
        rest,
        shares,
        others,
        slip,
        line(log_state),
        line(friction_a),
        line(friction_b),
        line(normal_stress),
        fluxes=lows[1:] + highs,
        rate=rate,
    )
    return (accel.reshape(-1), change.reshape(-1), rate)


def solution(mesh):
    placed = (
        P("slab"),
        P("slab"),
        P("slab"),
        P("slab"),
        P("slab"),
        P("slab"),
        P(None, "slab"),
        P(None, "slab"),
        P(("slab", "blk"), None, None, None),
        P(None, "slab"),
        P(None, "slab"),
        P(("slab", "blk")),
        P(("slab", "blk")),
        P(("slab", "blk")),
        P(None, None, ("slab", "blk")),
        P("slab", "blk", None),
        P("slab", "blk", None),
        P(),
    )

    return jax.shard_map(
        shards,
        mesh=mesh,
        in_specs=placed,
        out_specs=(P("slab"), P("slab"), P("slab", "blk", None)),
        check_vma=False,
    )
```
